32 devices in a mesh: section: 2 (over x), expert: 16 (over z, y, core).
Axes of the slice: x: 2, y: 2, z: 4, core: 2. Of those that a mesh axis runs over, the one named last changes fastest.
Arguments:
- images: bfloat16 [32, 256, 1408], P(('section', 'expert')), may hold values from -6 to 6
- norm_gain: bfloat16 [1408], replicated, may hold values from 0.5 to 1.5
- slot_map: bfloat16 [1408, 16], replicated, may hold values from -0.15625 to 0.15625
- logit_scale: float32 [1], replicated, may hold values from 30 to 80
- up_weight: bfloat16 [16, 5120, 1408], P('expert', 'section'), may hold values from -0.625 to 0.625
- down_weight: bfloat16 [16, 5120, 1408], P('expert', 'section'), may hold values from -0.3125 to 0.3125
Outputs:
- block_out: bfloat16 [32, 256, 1408], P(('section', 'expert'))
The draws below stay inside these ranges and needn't reach their ends.
All inputs are finite; a program needn't handle non-finite values.
Results may differ from the reference program's by a relative error of at most 0.011.
Values may be sent and summed in bfloat16 or wider, within the bound.
A program may use at most 64 MiB of HBM per device.

```python
import math
import jax
import jax.numpy as jnp
from jax import lax

D = 1408
FF = 5120
TOK = 256
EXPERTS = 16
IMAGES = 32


def levels(rng, extent, shards, low, top_value):
    def one(axis_at, shards_of):
        heights = jax.random.uniform(jax.random.fold_in(jax.random.fold_in(rng, 6), axis_at), (shards_of,), jnp.float32, low / len(shards), top_value / len(shards))
        return jnp.repeat(jnp.exp(heights), extent[axis_at] // shards_of).reshape((-1,) + (1,) * (len(extent) - axis_at - 1))

    loudness = one(*shards[0])
    for cut in shards[1:]:
        loudness = loudness * one(*cut)
    return loudness


def centred(own_key, extent, deviation, reach, split=(), kind=jnp.bfloat16):
    level = levels(own_key, extent, split, -0.22, 0.18) if split else 1.0
    result = jax.random.normal(own_key, extent, jnp.float32) * deviation * level
    return jnp.minimum(jnp.maximum(result, -reach), reach).astype(kind)


def setup_inputs(seed: int = 0) -> dict:
    key_list = jax.random.split(jax.random.key(seed), 7)
    images = centred(key_list[0], (IMAGES, TOK, D), 1.0, 6.0, ((0, 32),))
    norm_gain = jnp.clip(1.0 + 0.1 * jax.random.normal(key_list[1], (D,), jnp.float32), 0.5, 1.5).astype(jnp.bfloat16)
    slot_map = centred(key_list[2], (D, EXPERTS), D ** -0.5, 0.15625)
    logit_scale = jnp.clip(jnp.exp(jax.random.uniform(key_list[3], (1,), jnp.float32, math.log(30.0), math.log(80.0))), 30.0, 80.0)
    up_weight = centred(key_list[4], (EXPERTS, FF, D), (4.0 / D ** 0.5), 0.625, ((0, 16), (1, 2)))
    down_weight = centred(key_list[5], (EXPERTS, FF, D), (4.0 / FF ** 0.5), 0.3125, ((0, 16), (1, 2)))
    return dict(images=images, norm_gain=norm_gain, slot_map=slot_map, logit_scale=logit_scale, up_weight=up_weight, down_weight=down_weight)


epsilon = 1e-06

def normalize(inputs, gain_row):
    values = inputs.astype(jnp.float32)
    spread = lax.optimization_barrier(jnp.mean(values * values, axis=-1, keepdims=True))
    return (values * lax.rsqrt(spread + epsilon) * gain_row.astype(jnp.float32)).astype(jnp.bfloat16)

def weights_from(raw, normed, slot_cols, scale_now):
    values = normed.astype(jnp.float32)
    token_norm = jnp.sqrt(lax.optimization_barrier(jnp.sum(values * values, axis=-1)) + epsilon)
    columns = slot_cols.astype(jnp.float32)
    column_norm = jnp.sqrt(lax.optimization_barrier(jnp.sum(columns * columns, axis=0)) + epsilon)
    logits = scale_now * raw / (token_norm[:, None, :] * column_norm[None, :, None])
    scores = jnp.exp(logits)
    dispatch = (scores / lax.optimization_barrier(jnp.sum(scores, axis=-1, keepdims=True))).astype(jnp.bfloat16)
    combine = (scores / lax.optimization_barrier(jnp.sum(scores, axis=1, keepdims=True))).astype(jnp.bfloat16)
    return (dispatch, combine)

def reference(images, norm_gain, slot_map, logit_scale, up_weight, down_weight):
    normed = normalize(images, norm_gain)
    raw = jnp.einsum('itd,de->iet', normed.astype(jnp.float32), slot_map.astype(jnp.float32))
    dispatch, combine = weights_from(raw, normed, slot_map, logit_scale[0])
    slot_in = jnp.einsum('iet,itd->eid', dispatch.astype(jnp.float32), normed.astype(jnp.float32)).astype(jnp.bfloat16)
    hidden = jax.nn.gelu(jnp.einsum('eid,efd->eif', slot_in.astype(jnp.float32), up_weight.astype(jnp.float32))).astype(jnp.bfloat16)
    slot_out = jnp.einsum('eif,efd->eid', hidden.astype(jnp.float32), down_weight.astype(jnp.float32)).astype(jnp.bfloat16)
    mixed = jnp.einsum('iet,eid->itd', combine.astype(jnp.float32), slot_out.astype(jnp.float32))
    return (images.astype(jnp.float32) + mixed).astype(jnp.bfloat16)
```

```python
import functools

import jax
import jax.numpy as jnp
from jax import lax
from jax.experimental import pallas as pl
from jax.experimental.pallas import tpu as pltpu
from jax.sharding import PartitionSpec as P

epsilon = 1e-06
MESH = pl.DeviceIdType.MESH
NT = (((1,), (1,)), ((), ()))
TN = (((0,), (0,)), ((), ()))


def split_of(total, most, unit):
    best = unit
    for size in range(unit, most + 1, unit):
        if total % size == 0:
            best = size
    return best


def far_first(sections, experts):
    def distance(k):
        mask = k % experts
        return -(k // experts + mask // 4 + mask // 2 % 2)

    return sorted(range(1, sections * experts), key=distance)


def kernel(
    sections, experts, chunk,
    x_hbm, gain_hbm, slot_hbm, scale_hbm, up_hbm, down_hbm,
    out_v,
    gain_ref, slot_ref, scale_ref, xs, normed, stat, up_v, down_v, send1, recv1, send2, recv2,
    small_sem, x_sem, up_sem, down_sem, local_sem, send_sem, recv_sem,
):
    n = sections * experts
    tokens, width = xs.shape
    half = send1.shape[2]
    rest = width - half
    hidden_units = up_v.shape[0]
    chunks = hidden_units // chunk
    section = lax.axis_index("section")
    expert = lax.axis_index("expert")
    me = section * experts + expert

    x_parts = x_sem.shape[0]
    x_rows = tokens // x_parts
    x_copies = [
        pltpu.make_async_copy(
            x_hbm.at[pl.ds(i * x_rows, x_rows)], xs.at[pl.ds(i * x_rows, x_rows)], x_sem.at[i]
        )
        for i in range(x_parts)
    ]
    small_copies = [
        pltpu.make_async_copy(source, target, small_sem.at[i])
        for i, (source, target) in enumerate(
            [(gain_hbm, gain_ref), (slot_hbm, slot_ref), (scale_hbm, scale_ref)]
        )
    ]

    barrier = pltpu.get_barrier_semaphore()

    def wrapped(value, bound):
        return jnp.where(value >= bound, value - bound, value)

    def visit_at(k, visit):
        s = wrapped(section + k // experts, sections)
        mask = k % experts
        e = jnp.bitwise_xor(expert, mask) if paired else wrapped(expert + mask, experts)
        visit(s * experts + e, e, {"section": s, "expert": e})

    paired = experts & (experts - 1) == 0
    order = far_first(sections, experts)

    def for_others(visit, between=None):
        if n <= 64:
            for at, k in enumerate(order):
                if at == 8 and between is not None:
                    between()
                visit_at(k, visit)
        else:
            if between is not None:
                between()

            def step(k, carry):
                visit_at(k, visit)
                return carry

            lax.fori_loop(1, n, step, 0)

    def greet(target, e, device):
        pl.semaphore_signal(barrier, inc=1, device_id=device, device_id_type=MESH)

    def start_inputs():
        for copy in x_copies + small_copies:
            copy.start()

    for_others(greet, start_inputs)

    up_copies = []
    down_copies = []
    for c in range(chunks):
        rows = pl.ds(c * chunk, chunk)
        up_copies.append(pltpu.make_async_copy(up_hbm.at[rows], up_v.at[rows], up_sem.at[c]))
        down_copies.append(pltpu.make_async_copy(down_hbm.at[rows], down_v.at[rows], down_sem.at[c]))
    for copy in up_copies + down_copies:
        copy.start()

    for copy in small_copies:
        copy.wait()
    columns = slot_ref[...].astype(jnp.float32)
    column_norm = jnp.sqrt(jnp.sum(columns * columns, axis=-1, keepdims=True) + epsilon)
    gain = gain_ref[...].astype(jnp.float32).reshape(1, width)

    step_rows = 16

    def norm_step(i, carry):
        rows = pl.ds(pl.multiple_of(i * step_rows, step_rows), step_rows)
        values = xs[rows, :].astype(jnp.float32)
        spread = jnp.sum(values * values, axis=-1, keepdims=True) * (1.0 / width)
        result = (values * lax.rsqrt(spread + epsilon) * gain).astype(jnp.bfloat16)
        normed[rows, :] = result
        wide = result.astype(jnp.float32)
        square = jnp.sum(wide * wide, axis=-1, keepdims=True)
        stat[rows, :] = jnp.broadcast_to(square, (step_rows, stat.shape[1]))
        return carry

    per = x_rows // step_rows
    for i, copy in enumerate(x_copies):
        copy.wait()
        lax.fori_loop(i * per, (i + 1) * per, norm_step, 0, unroll=True)

    raw = lax.dot_general(slot_ref[...], normed[...], NT, preferred_element_type=jnp.float32)
    token_norm = jnp.sqrt(jnp.transpose(stat[...])[0:1, :] + epsilon)
    logits = scale_ref[0] * raw / (token_norm * column_norm)
    scores = jnp.exp(logits)
    dispatch = (scores / jnp.sum(scores, axis=1, keepdims=True)).astype(jnp.bfloat16)
    combine = (scores / jnp.sum(scores, axis=0, keepdims=True)).astype(jnp.bfloat16)
    slot_in = jnp.dot(dispatch, normed[...], preferred_element_type=jnp.float32).astype(jnp.bfloat16)
    send1[:, 0, :] = slot_in[:, :half]
    send1[:, 1, :rest] = slot_in[:, half:]

    pl.semaphore_wait(barrier, n - 1)

    own1 = pltpu.make_async_copy(send1.at[expert], recv1.at[me], local_sem.at[0])
    own1.start()

    def dispatch_row(target, e, device):
        pltpu.make_async_remote_copy(
            src_ref=send1.at[e], dst_ref=recv1.at[me], send_sem=send_sem.at[0], recv_sem=recv_sem.at[0],
            device_id=device, device_id_type=MESH,
        ).start()

    for_others(dispatch_row)

    def wait_all(buffer, sem):
        part = buffer.at[pl.ds(0, n - 1)]
        pltpu.make_async_copy(part, part, sem).wait()

    own1.wait()
    wait_all(recv1, recv_sem.at[0])
    left = recv1[:, 0, :]
    right = recv1[:, 1, :rest]
    rows_in = jnp.concatenate([left, right], axis=1)
    total = None
    for c in range(chunks):
        rows = pl.ds(c * chunk, chunk)
        up_copies[c].wait()
        pre = lax.dot_general(rows_in, up_v[rows, :], NT, preferred_element_type=jnp.float32)
        act = jax.nn.gelu(pre).astype(jnp.bfloat16)
        down_copies[c].wait()
        term = jnp.dot(act, down_v[rows, :], preferred_element_type=jnp.float32)
        total = term if total is None else total + term
    partial = total.astype(jnp.bfloat16)
    send2[:, 0, :] = partial[:, :half]
    send2[:, 1, :rest] = partial[:, half:]

    own2 = pltpu.make_async_copy(send2.at[me], recv2.at[me], local_sem.at[1])
    own2.start()

    def return_row(target, e, device):
        pltpu.make_async_remote_copy(
            src_ref=send2.at[target], dst_ref=recv2.at[me], send_sem=send_sem.at[1], recv_sem=recv_sem.at[1],
            device_id=device, device_id_type=MESH,
        ).start()

    for_others(return_row)

    own2.wait()
    wait_all(recv2, recv_sem.at[1])
    summed = recv2[pl.ds(0, experts)].astype(jnp.float32)
    for s in range(1, sections):
        summed = summed + recv2[pl.ds(s * experts, experts)].astype(jnp.float32)
    slot_out = summed.astype(jnp.bfloat16)
    slot_out = jnp.concatenate([slot_out[:, 0, :], slot_out[:, 1, :rest]], axis=1)

    o_parts = 4
    o_rows = tokens // o_parts
    for i in range(o_parts):
        rows = pl.ds(i * o_rows, o_rows)
        mixed = lax.dot_general(
            combine[:, i * o_rows:(i + 1) * o_rows], slot_out, TN, preferred_element_type=jnp.float32
        )
        out_v[rows, :] = (xs[rows, :].astype(jnp.float32) + mixed).astype(jnp.bfloat16)
    wait_all(recv1, send_sem.at[0])
    wait_all(recv2, send_sem.at[1])


def solution(mesh):
    sections, experts = mesh.shape["section"], mesh.shape["expert"]
    n = sections * experts

    def local(images, norm_gain, slot_map, logit_scale, up_weight, down_weight):
        count, tokens, width = images.shape
        held, hidden_units, _ = up_weight.shape
        slots = slot_map.shape[1]
        assert count == 1 and held == 1 and slots == experts
        half = -(-width // 256) * 128
        chunk = split_of(hidden_units, 1280, 128)
        chunks = hidden_units // chunk
        bf16 = jnp.bfloat16
        hbm = pl.BlockSpec(memory_space=pl.ANY)
        vmem = pl.BlockSpec(memory_space=pltpu.VMEM)
        x_parts = 4
        result = pl.pallas_call(
            functools.partial(kernel, sections, experts, chunk),
            out_shape=pltpu.VMEM((tokens, width), bf16),
            in_specs=[hbm, hbm, hbm, pl.BlockSpec(memory_space=pltpu.HBM), hbm, hbm],
            out_specs=vmem,
            scratch_shapes=[
                pltpu.VMEM((width,), bf16),
                pltpu.VMEM((slots, width), bf16),
                pltpu.SMEM((1,), jnp.float32),
                pltpu.VMEM((tokens, width), bf16),
                pltpu.VMEM((tokens, width), bf16),
                pltpu.VMEM((tokens, 128), jnp.float32),
                pltpu.VMEM((hidden_units, width), bf16),
                pltpu.VMEM((hidden_units, width), bf16),
                pltpu.VMEM((experts, 2, half), bf16),
                pltpu.VMEM((n, 2, half), bf16),
                pltpu.VMEM((n, 2, half), bf16),
                pltpu.VMEM((n, 2, half), bf16),
                pltpu.SemaphoreType.DMA((3,)),
                pltpu.SemaphoreType.DMA((x_parts,)),
                pltpu.SemaphoreType.DMA((chunks,)),
                pltpu.SemaphoreType.DMA((chunks,)),
                pltpu.SemaphoreType.DMA((2,)),
                pltpu.SemaphoreType.DMA((2,)),
                pltpu.SemaphoreType.DMA((2,)),
            ],
            compiler_params=pltpu.CompilerParams(
                collective_id=0, has_side_effects=True, vmem_limit_bytes=60 * 1024 * 1024
            ),
        )(
            images.reshape(tokens, width), norm_gain, slot_map.T, logit_scale,
            up_weight.reshape(hidden_units, width), down_weight.reshape(hidden_units, width),
        )
        return result.reshape(1, tokens, width)

    return jax.shard_map(
        local,
        mesh=mesh,
        in_specs=(
            P(("section", "expert"), None, None),
            P(),
            P(),
            P(),
            P("expert", "section", None),
            P("expert", "section", None),
        ),
        out_specs=P(("section", "expert"), None, None),
        check_vma=False,
    )
```

```python
import functools

import jax
import jax.numpy as jnp
from jax import lax
from jax.experimental import pallas as pl
from jax.experimental.pallas import tpu as pltpu
from jax.sharding import PartitionSpec as P

epsilon = 1e-06
MESH = pl.DeviceIdType.MESH
NT = (((1,), (1,)), ((), ()))
TN = (((0,), (0,)), ((), ()))
U = 256
STRIP = 16


def split_of(total, most, unit):
    best = unit
    for size in range(unit, most + 1, unit):
        if total % size == 0:
            best = size
    return best


def far_first(sections, experts):
    def distance(k):
        mask = k % experts
        return -(k // experts + mask // 4 + mask // 2 % 2)

    return sorted(range(1, sections * experts), key=distance)


def swap_pairs(v, even):
    return jnp.where(even, pltpu.roll(v, v.shape[0] - 1, 0), pltpu.roll(v, 1, 0))

def gelu(x):
    k = 0.7978845608028654
    return (0.5 * x) * (1.0 + jnp.tanh(x * (k + (k * 0.044715) * (x * x))))

def expert_mlp(rows_ref, upt_v, down_v, act_v, out_ref, ups, downs, halves, half, width, lag=2):
    M = rows_ref.shape[0]
    hidden = upt_v.shape[1]
    bf16 = jnp.bfloat16
    right = width - half
    blocks = hidden // U // 2
    rem = right % U
    tiles = [(0, j * U) for j in range(half // U)] + [(1, j * U) for j in range(right // U)]
    tail = right // U * U
    strips = M // STRIP
    even = lax.broadcasted_iota(jnp.int32, (M, U), 0) % 2 == 0
    even_strip = lax.broadcasted_iota(jnp.int32, (STRIP, U), 0) % 2 == 0
    zero = jnp.zeros((M, U), bf16)
    slot = [0, 0]

    def piece(s):
        return slice(s * STRIP, (s + 1) * STRIP)

    def feed(q, tile, accs, operands):
        r = slot[q]
        slot[q] = 1 - r
        pltpu.matmul_push_rhs(tile, r, q)
        first = True
        for acc, operand in zip(accs, operands):
            for s in range(strips):
                pltpu.matmul_acc_lhs(acc[s], operand[piece(s)], load_staged_rhs=r if first else None)
                first = False

    def at_block(q, b):
        return pl.ds((q * blocks + b) * U, U)

    lhs = []
    for side, at in tiles:
        v = rows_ref[:, at:at + U]
        lhs.append(jnp.where(even, v, zero) if side == 0 else jnp.where(even, zero, v))
    if rem:
        v = rows_ref[:, tail:tail + rem]
        v = jnp.where(even[:, :rem], zero[:, :rem], v)
        lhs_tail = [jnp.concatenate([v, zero[:, :rem]], axis=1), jnp.concatenate([zero[:, :rem], v], axis=1)]

    def finish(q, b, s):
        pre = pltpu.matmul_pop(ups[q][b][s])
        pre = pre + swap_pairs(pre, even_strip)
        act_v[piece(s), at_block(q, b)] = gelu(pre).astype(bf16)

    pending = []

    def drain(count):
        for _ in range(min(count, len(pending))):
            pending.pop(0)()

    def up_block(b, rate):
        for side_at, operand in zip(tiles, lhs):
            side, at = side_at
            for q in range(2):
                feed(q, upt_v[pl.ds(side * half + at, U), at_block(q, b)], [ups[q][b]], [operand])
            drain(rate)
        done = []
        if rem:
            k = pl.ds(half + tail, rem)
            if b % 2 == 1:
                for q in range(2):
                    pair = jnp.concatenate([upt_v[k, at_block(q, b - 1)], upt_v[k, at_block(q, b)]], axis=0)
                    feed(q, pair, [ups[q][b - 1], ups[q][b]], lhs_tail)
                done = [b - 1, b]
            elif b == blocks - 1:
                for q in range(2):
                    one = upt_v[k, at_block(q, b)]
                    feed(q, jnp.concatenate([one, one], axis=0), [ups[q][b]], lhs_tail[:1])
                done = [b]
        else:
            done = [b]
        for d in done:
            for s in range(strips):
                for q in range(2):
                    pending.append(lambda q=q, d=d, s=s: finish(q, d, s))

    for b in range(blocks):
        up_block(b, lag)

    def act(q, b):
        return act_v[:, at_block(q, b)]

    def down_step(j, b):
        side, at = tiles[j]
        for q in range(2):
            feed(q, down_v[at_block(q, b), pl.ds(side * half + at, U)], [downs[q][j]], [act(q, b)])

    def down_tail(pair):
        cols = pl.ds(half + tail, rem)
        for q in range(2):
            v = [down_v[at_block(q, b), cols] for b in pair]
            if len(v) == 1:
                v = v * 2
            feed(q, jnp.concatenate(v, axis=1), [halves[q][i] for i in range(len(pair))], [act(q, b) for b in pair])

    nl, nr = half // U, right // U
    pairs = [list(range(b, min(b + 2, blocks))) for b in range(0, blocks, 2)]

    def total(group, s):
        return pltpu.matmul_pop(group[0][s]) + pltpu.matmul_pop(group[1][s])

    def emit(j, s):
        l = total([downs[0][j], downs[1][j]], s)
        rows = piece(s)
        if j < nr:
            r = total([downs[0][nl + j], downs[1][nl + j]], s)
            out_ref[rows, j * U:(j + 1) * U] = jnp.where(even_strip, l, r).astype(bf16)
        elif rem:
            r = total([halves[0][0], halves[1][0]], s)[:, :rem] + total([halves[0][1], halves[1][1]], s)[:, rem:]
            both = jnp.where(even_strip[:, :rem], l[:, :rem], r)
            out_ref[rows, j * U:(j + 1) * U] = jnp.concatenate([both, l[:, rem:]], axis=1).astype(bf16)
        else:
            out_ref[rows, j * U:(j + 1) * U] = l.astype(bf16)

    ready = blocks - 1 if blocks % 2 else blocks - 2
    groups = []
    for j in reversed(range(nl)):
        groups.append((j, [j] + ([nl + j] if j < nr else [])))
    first = True
    for j, columns in groups:
        tails = rem and j >= nr
        for b in range(blocks):
            if first and b == ready:
                drain(len(pending))
            for c in columns:
                down_step(c, b)
                drain(lag)
            if tails and (b % 2 == 1 or b == blocks - 1):
                down_tail(pairs[b // 2])
                drain(lag)
        drain(len(pending))
        first = False
        for s in range(strips):
            pending.append(lambda j=j, s=s: emit(j, s))
    drain(len(pending))

def routing_kernel(
    sections, experts, half,
    x_hbm, gain_hbm, slot_hbm, scale_ref, up_hbm, down_hbm,
    xs, back, mix_left, mix_right,
    gain_ref, slot_ref, normed, stat, up_v, upt_v, down_v, act_v, send1, recv1, send2, recv2, sized,
    small_sem, x_sem, up_sem, down_sem, local_sem, send_sem, recv_sem,
):
    tokens, width = xs.shape
    slots = slot_ref.shape[0]
    padded = normed.shape[1]
    columns = padded // U
    images = sections * experts

    def spec(rows):
        return lambda q: [pltpu.ACC(q)((STRIP, U), jnp.float32) for _ in range(rows // STRIP)]

    def per_unit(count, rows):
        make = spec(rows)
        return [[make(q) for _ in range(count)] for q in range(2)]

    hidden = up_v.shape[0]
    wide = half // U + (width - half) // U

    def run(raws, ins, ups, downs, halves):
        routing_body(
            sections, experts, half,
            x_hbm, gain_hbm, slot_hbm, scale_ref, up_hbm, down_hbm,
            xs, back, mix_left, mix_right,
            gain_ref, slot_ref, normed, stat, up_v, upt_v, down_v, act_v, send1, recv1, send2, recv2, sized,
            small_sem, x_sem, up_sem, down_sem, local_sem, send_sem, recv_sem,
            raws, ins, ups, downs, halves,
        )

    pl.run_scoped(
        run,
        [pltpu.ACC(q)((slots, U), jnp.float32) for q in range(2)],
        [pltpu.ACC(t % 2)((2 * slots, U), jnp.float32) for t in range(columns)],
        per_unit(hidden // U // 2, 2 * images),
        per_unit(wide, 2 * images),
        per_unit(2, 2 * images),
    )


def routing_body(
    sections, experts, half,
    x_hbm, gain_hbm, slot_hbm, scale_ref, up_hbm, down_hbm,
    xs, back, mix_left, mix_right,
    gain_ref, slot_ref, normed, stat, up_v, upt_v, down_v, act_v, send1, recv1, send2, recv2, sized,
    small_sem, x_sem, up_sem, down_sem, local_sem, send_sem, recv_sem,
    raws, ins, ups, downs, halves,
):
    n = sections * experts
    tokens, width = xs.shape
    slots = slot_ref.shape[0]
    padded = normed.shape[1]
    hidden = up_v.shape[0]
    bf16 = jnp.bfloat16
    section = lax.axis_index("section")
    expert = lax.axis_index("expert")
    me = section * experts + expert

    x_parts = x_sem.shape[0]
    x_rows = tokens // x_parts
    x_copies = [
        pltpu.make_async_copy(
            x_hbm.at[pl.ds(i * x_rows, x_rows)], xs.at[pl.ds(i * x_rows, x_rows)], x_sem.at[i]
        )
        for i in range(x_parts)
    ]
    small_copies = [
        pltpu.make_async_copy(gain_hbm, gain_ref, small_sem.at[0]),
        pltpu.make_async_copy(slot_hbm, slot_ref, small_sem.at[1]),
    ]

    barrier = pltpu.get_barrier_semaphore()

    def for_others(visit, between=None):
        for at, k in enumerate(far_first(sections, experts)):
            if at == 8 and between is not None:
                between()
            s = lax.rem(section + k // experts, sections)
            e = jnp.bitwise_xor(expert, k % experts)
            visit(s * experts + e, e, {"section": s, "expert": e})

    def greet(target, e, device):
        pl.semaphore_signal(barrier, inc=1, device_id=device, device_id_type=MESH)

    def start_inputs():
        for copy in x_copies + small_copies:
            copy.start()

    for_others(greet, start_inputs)

    up_parts, down_parts = up_sem.shape[0], down_sem.shape[0]
    up_rows, down_rows = hidden // up_parts, hidden // down_parts

    def up_copy(c):
        rows = pl.ds(pl.multiple_of(c * up_rows, up_rows), up_rows)
        return pltpu.make_async_copy(up_hbm.at[rows], up_v.at[rows], up_sem.at[c])

    def down_copy(c):
        rows = pl.ds(c * down_rows, down_rows)
        return pltpu.make_async_copy(down_hbm.at[rows], down_v.at[rows], down_sem.at[c])

    for c in range(up_parts):
        up_copy(c).start()
    for c in range(down_parts):
        down_copy(c).start()

    for copy in small_copies:
        copy.wait()
    slot_rows = slot_ref[...]
    slot_wide = slot_rows.astype(jnp.float32)
    column_norm = jnp.sqrt(jnp.sum(slot_wide * slot_wide, axis=-1, keepdims=True) + epsilon)
    gain = gain_ref[...].astype(jnp.float32).reshape(1, width)
    if padded > width:
        normed[:, width:] = jnp.zeros((tokens, padded - width), bf16)
        slot_rows = jnp.concatenate([slot_rows, jnp.zeros((slots, padded - width), bf16)], axis=1)

    step_rows = 16

    def norm_step(i, carry):
        rows = pl.ds(pl.multiple_of(i * step_rows, step_rows), step_rows)
        values = xs[rows, :].astype(jnp.float32)
        spread = jnp.sum(values * values, axis=-1, keepdims=True) * (1.0 / width)
        result = (values * lax.rsqrt(spread + epsilon) * gain).astype(bf16)
        normed[rows, :width] = result
        wide = result.astype(jnp.float32)
        square = jnp.sum(wide * wide, axis=-1, keepdims=True)
        stat[rows, :] = jnp.broadcast_to(square, (step_rows, stat.shape[1]))
        return carry

    per = x_rows // step_rows
    for i, copy in enumerate(x_copies):
        copy.wait()
        lax.fori_loop(i * per, (i + 1) * per, norm_step, 0, unroll=True)

    tiles = padded // U
    for t in range(tiles):
        q, r = t % 2, t // 2 % 2
        pltpu.matmul_push_rhs(normed[:, t * U:(t + 1) * U], r, q, transpose=True)
        pltpu.matmul_acc_lhs(raws[q], slot_rows[:, t * U:(t + 1) * U], load_staged_rhs=r)
    raw = pltpu.matmul_pop(raws[0]) + pltpu.matmul_pop(raws[1])
    token_norm = jnp.sqrt(jnp.transpose(stat[...])[0:1, :] + epsilon)
    logits = scale_ref[0] * raw / (token_norm * column_norm)
    scores = jnp.exp(logits)
    dispatch = scores / jnp.sum(scores, axis=1, keepdims=True)
    combine = scores / jnp.sum(scores, axis=0, keepdims=True)
    dispatch = jnp.repeat(dispatch, 2, axis=0).astype(bf16)
    even = lax.broadcasted_iota(jnp.int32, (2 * slots, U), 0) % 2 == 0
    shift = tiles // 2
    for j in range(shift):
        for t in (j, j + shift):
            q, r = t % 2, t // 2 % 2
            pltpu.matmul_push_rhs(normed[:, t * U:(t + 1) * U], r, q)
            pltpu.matmul_acc_lhs(ins[t], dispatch, load_staged_rhs=r)
    for j in range(shift):
        left, right = pltpu.matmul_pop(ins[j]), pltpu.matmul_pop(ins[j + shift])
        send1[:, j * U:(j + 1) * U] = jnp.where(even, left, right).astype(bf16)

    pl.semaphore_wait(barrier, n - 1)

    def pair(index):
        return pl.ds(pl.multiple_of(2 * index, 2), 2)

    def send_rows(source, target, i, by_expert):
        def visit(index, e, device):
            pltpu.make_async_remote_copy(
                src_ref=source.at[pair(e if by_expert else index)], dst_ref=target.at[pair(me)],
                send_sem=send_sem.at[i], recv_sem=recv_sem.at[i],
                device_id=device, device_id_type=MESH,
            ).start()

        for_others(visit)

    def wait_all(sem):
        pltpu.make_async_copy(sized, sized, sem).wait()

    send_rows(send1, recv1, 0, True)
    own1 = pltpu.make_async_copy(send1.at[pair(expert)], recv1.at[pair(me)], local_sem.at[0])
    own1.start()

    stacked = jnp.concatenate([jnp.repeat(combine, 2, axis=0)] * sections, axis=0)
    by_token = jnp.transpose(stacked)
    lane_even = lax.broadcasted_iota(jnp.int32, by_token.shape, 1) % 2 == 0
    mix_left[...] = jnp.where(lane_even, by_token, 0.0).astype(bf16)
    mix_right[...] = jnp.where(lane_even, 0.0, by_token).astype(bf16)

    def turn(c, carry):
        up_copy(c).wait()
        at = pl.multiple_of(c * up_rows, up_rows)
        for k in range(0, width, 128):
            upt_v[k:k + 128, pl.ds(at, up_rows)] = up_v[pl.ds(at, up_rows), k:k + 128].T
        return carry

    lax.fori_loop(0, up_parts, turn, 0)
    for c in range(down_parts):
        down_copy(c).wait()

    own1.wait()
    wait_all(recv_sem.at[0])
    expert_mlp(recv1, upt_v, down_v, act_v, send2, ups, downs, halves, half, width)

    send_rows(send2, recv2, 1, False)
    own2 = pltpu.make_async_copy(send2.at[pair(me)], recv2.at[pair(me)], local_sem.at[1])
    own2.start()
    wait_all(send_sem.at[0])
    own2.wait()
    wait_all(recv_sem.at[1])
    back[...] = recv2[...]
    wait_all(send_sem.at[1])


def mixing_kernel(half, xs, back, mix_left, mix_right, out_hbm, out_v, sem):
    tokens, width = xs.shape
    parts = sem.shape[0]
    rows_each = tokens // parts
    copies = []
    for i in range(parts):
        rows = pl.ds(i * rows_each, rows_each)
        left = jnp.dot(mix_left[rows, :], back[...], preferred_element_type=jnp.float32)
        right = jnp.dot(mix_right[rows, :], back[:, :width - half], preferred_element_type=jnp.float32)
        out_v[rows, :half] = (xs[rows, :half].astype(jnp.float32) + left).astype(jnp.bfloat16)
        out_v[rows, half:] = (xs[rows, half:].astype(jnp.float32) + right).astype(jnp.bfloat16)
        copy = pltpu.make_async_copy(out_v.at[rows], out_hbm.at[rows], sem.at[i])
        copy.start()
        copies.append(copy)
    for copy in copies:
        copy.wait()


def fast_call(sections, experts, half, images, norm_gain, slot_map, logit_scale, up_weight, down_weight):
    tokens, width = images.shape
    hidden = up_weight.shape[0]
    slots = slot_map.shape[0]
    n = sections * experts
    padded = -(-width // (2 * U)) * 2 * U
    bf16 = jnp.bfloat16
    hbm = pl.BlockSpec(memory_space=pl.ANY)
    vmem = pl.BlockSpec(memory_space=pltpu.VMEM)
    x_parts, up_parts, down_parts, out_parts = 4, hidden // U, 2, 4
    xs, back, mix_left, mix_right = pl.pallas_call(
        functools.partial(routing_kernel, sections, experts, half),
        out_shape=[
            pltpu.VMEM((tokens, width), bf16),
            pltpu.VMEM((2 * n, half), bf16),
            pltpu.VMEM((tokens, 2 * n), bf16),
            pltpu.VMEM((tokens, 2 * n), bf16),
        ],
        in_specs=[hbm, hbm, hbm, pl.BlockSpec(memory_space=pltpu.SMEM), hbm, hbm],
        out_specs=[vmem] * 4,
        scratch_shapes=[
            pltpu.VMEM((width,), bf16),
            pltpu.VMEM((slots, width), bf16),
            pltpu.VMEM((tokens, padded), bf16),
            pltpu.VMEM((tokens, 128), jnp.float32),
            pltpu.VMEM((hidden, width), bf16),
            pltpu.VMEM((width, hidden), bf16),
            pltpu.VMEM((hidden, width), bf16),
            pltpu.VMEM((2 * n, hidden), bf16),
            pltpu.VMEM((2 * slots, half), bf16),
            pltpu.VMEM((2 * n, half), bf16),
            pltpu.VMEM((2 * n, half), bf16),
            pltpu.VMEM((2 * n, half), bf16),
            pltpu.VMEM((n - 1, 2, half), bf16),
            pltpu.SemaphoreType.DMA((2,)),
            pltpu.SemaphoreType.DMA((x_parts,)),
            pltpu.SemaphoreType.DMA((up_parts,)),
            pltpu.SemaphoreType.DMA((down_parts,)),
            pltpu.SemaphoreType.DMA((2,)),
            pltpu.SemaphoreType.DMA((2,)),
            pltpu.SemaphoreType.DMA((2,)),
        ],
        compiler_params=pltpu.CompilerParams(
            collective_id=0, has_side_effects=True, vmem_limit_bytes=60 * 1024 * 1024
        ),
    )(images, norm_gain, slot_map, logit_scale, up_weight, down_weight)
    return pl.pallas_call(
        functools.partial(mixing_kernel, half),
        out_shape=jax.ShapeDtypeStruct((tokens, width), bf16),
        in_specs=[vmem] * 4,
        out_specs=hbm,
        scratch_shapes=[pltpu.VMEM((tokens, width), bf16), pltpu.SemaphoreType.DMA((out_parts,))],
    )(*(pltpu.with_memory_space_constraint(v, pltpu.VMEM) for v in (xs, back, mix_left, mix_right)))


def general_kernel(
    sections, experts, chunk,
    x_hbm, gain_hbm, slot_hbm, scale_hbm, up_hbm, down_hbm,
    out_v,
    gain_ref, slot_ref, scale_ref, xs, normed, stat, up_v, down_v, send1, recv1, send2, recv2,
    small_sem, x_sem, up_sem, down_sem, local_sem, send_sem, recv_sem,
):
    n = sections * experts
    tokens, width = xs.shape
    half = send1.shape[2]
    rest = width - half
    hidden_units = up_v.shape[0]
    chunks = hidden_units // chunk
    section = lax.axis_index("section")
    expert = lax.axis_index("expert")
    me = section * experts + expert

    x_parts = x_sem.shape[0]
    x_rows = tokens // x_parts
    x_copies = [
        pltpu.make_async_copy(
            x_hbm.at[pl.ds(i * x_rows, x_rows)], xs.at[pl.ds(i * x_rows, x_rows)], x_sem.at[i]
        )
        for i in range(x_parts)
    ]
    small_copies = [
        pltpu.make_async_copy(source, target, small_sem.at[i])
        for i, (source, target) in enumerate(
            [(gain_hbm, gain_ref), (slot_hbm, slot_ref), (scale_hbm, scale_ref)]
        )
    ]

    barrier = pltpu.get_barrier_semaphore()

    def wrapped(value, bound):
        return jnp.where(value >= bound, value - bound, value)

    def visit_at(k, visit):
        s = wrapped(section + k // experts, sections)
        mask = k % experts
        e = jnp.bitwise_xor(expert, mask) if paired else wrapped(expert + mask, experts)
        visit(s * experts + e, e, {"section": s, "expert": e})

    paired = experts & (experts - 1) == 0
    order = far_first(sections, experts)

    def for_others(visit, between=None):
        if n <= 64:
            for at, k in enumerate(order):
                if at == 8 and between is not None:
                    between()
                visit_at(k, visit)
        else:
            if between is not None:
                between()

            def step(k, carry):
                visit_at(k, visit)
                return carry

            lax.fori_loop(1, n, step, 0)

    def greet(target, e, device):
        pl.semaphore_signal(barrier, inc=1, device_id=device, device_id_type=MESH)

    def start_inputs():
        for copy in x_copies + small_copies:
            copy.start()

    for_others(greet, start_inputs)

    up_copies = []
    down_copies = []
    for c in range(chunks):
        rows = pl.ds(c * chunk, chunk)
        up_copies.append(pltpu.make_async_copy(up_hbm.at[rows], up_v.at[rows], up_sem.at[c]))
        down_copies.append(pltpu.make_async_copy(down_hbm.at[rows], down_v.at[rows], down_sem.at[c]))
    for copy in up_copies + down_copies:
        copy.start()

    for copy in small_copies:
        copy.wait()
    columns = slot_ref[...].astype(jnp.float32)
    column_norm = jnp.sqrt(jnp.sum(columns * columns, axis=-1, keepdims=True) + epsilon)
    gain = gain_ref[...].astype(jnp.float32).reshape(1, width)

    step_rows = 16

    def norm_step(i, carry):
        rows = pl.ds(pl.multiple_of(i * step_rows, step_rows), step_rows)
        values = xs[rows, :].astype(jnp.float32)
        spread = jnp.sum(values * values, axis=-1, keepdims=True) * (1.0 / width)
        result = (values * lax.rsqrt(spread + epsilon) * gain).astype(jnp.bfloat16)
        normed[rows, :] = result
        wide = result.astype(jnp.float32)
        square = jnp.sum(wide * wide, axis=-1, keepdims=True)
        stat[rows, :] = jnp.broadcast_to(square, (step_rows, stat.shape[1]))
        return carry

    per = x_rows // step_rows
    for i, copy in enumerate(x_copies):
        copy.wait()
        lax.fori_loop(i * per, (i + 1) * per, norm_step, 0, unroll=True)

    raw = lax.dot_general(slot_ref[...], normed[...], NT, preferred_element_type=jnp.float32)
    token_norm = jnp.sqrt(jnp.transpose(stat[...])[0:1, :] + epsilon)
    logits = scale_ref[0] * raw / (token_norm * column_norm)
    scores = jnp.exp(logits)
    dispatch = (scores / jnp.sum(scores, axis=1, keepdims=True)).astype(jnp.bfloat16)
    combine = (scores / jnp.sum(scores, axis=0, keepdims=True)).astype(jnp.bfloat16)
    slot_in = jnp.dot(dispatch, normed[...], preferred_element_type=jnp.float32).astype(jnp.bfloat16)
    send1[:, 0, :] = slot_in[:, :half]
    send1[:, 1, :rest] = slot_in[:, half:]

    pl.semaphore_wait(barrier, n - 1)

    own1 = pltpu.make_async_copy(send1.at[expert], recv1.at[me], local_sem.at[0])
    own1.start()

    def dispatch_row(target, e, device):
        pltpu.make_async_remote_copy(
            src_ref=send1.at[e], dst_ref=recv1.at[me], send_sem=send_sem.at[0], recv_sem=recv_sem.at[0],
            device_id=device, device_id_type=MESH,
        ).start()

    for_others(dispatch_row)

    def wait_all(buffer, sem):
        part = buffer.at[pl.ds(0, n - 1)]
        pltpu.make_async_copy(part, part, sem).wait()

    own1.wait()
    wait_all(recv1, recv_sem.at[0])
    left = recv1[:, 0, :]
    right = recv1[:, 1, :rest]
    rows_in = jnp.concatenate([left, right], axis=1)
    total = None
    for c in range(chunks):
        rows = pl.ds(c * chunk, chunk)
        up_copies[c].wait()
        pre = lax.dot_general(rows_in, up_v[rows, :], NT, preferred_element_type=jnp.float32)
        act = jax.nn.gelu(pre).astype(jnp.bfloat16)
        down_copies[c].wait()
        term = jnp.dot(act, down_v[rows, :], preferred_element_type=jnp.float32)
        total = term if total is None else total + term
    partial = total.astype(jnp.bfloat16)
    send2[:, 0, :] = partial[:, :half]
    send2[:, 1, :rest] = partial[:, half:]

    own2 = pltpu.make_async_copy(send2.at[me], recv2.at[me], local_sem.at[1])
    own2.start()

    def return_row(target, e, device):
        pltpu.make_async_remote_copy(
            src_ref=send2.at[target], dst_ref=recv2.at[me], send_sem=send_sem.at[1], recv_sem=recv_sem.at[1],
            device_id=device, device_id_type=MESH,
        ).start()

    for_others(return_row)

    own2.wait()
    wait_all(recv2, recv_sem.at[1])
    summed = recv2[pl.ds(0, experts)].astype(jnp.float32)
    for s in range(1, sections):
        summed = summed + recv2[pl.ds(s * experts, experts)].astype(jnp.float32)
    slot_out = summed.astype(jnp.bfloat16)
    slot_out = jnp.concatenate([slot_out[:, 0, :], slot_out[:, 1, :rest]], axis=1)

    o_parts = 4
    o_rows = tokens // o_parts
    for i in range(o_parts):
        rows = pl.ds(i * o_rows, o_rows)
        mixed = lax.dot_general(
            combine[:, i * o_rows:(i + 1) * o_rows], slot_out, TN, preferred_element_type=jnp.float32
        )
        out_v[rows, :] = (xs[rows, :].astype(jnp.float32) + mixed).astype(jnp.bfloat16)
    wait_all(recv1, send_sem.at[0])
    wait_all(recv2, send_sem.at[1])


def solution(mesh):
    sections, experts = mesh.shape["section"], mesh.shape["expert"]
    n = sections * experts

    def local(images, norm_gain, slot_map, logit_scale, up_weight, down_weight):
        count, tokens, width = images.shape
        held, hidden_units, _ = up_weight.shape
        slots = slot_map.shape[1]
        assert count == 1 and held == 1 and slots == experts
        half = -(-width // 256) * 128
        chunk = split_of(hidden_units, 1280, 128)
        chunks = hidden_units // chunk
        bf16 = jnp.bfloat16
        hbm = pl.BlockSpec(memory_space=pl.ANY)
        vmem = pl.BlockSpec(memory_space=pltpu.VMEM)
        fits = (
            tokens == U and slots % STRIP == 0 and experts & (experts - 1) == 0 and 2 * n <= 64
            and half % U == 0 and 2 * half - width < U and hidden_units % (2 * U) == 0
        )
        if fits:
            result = fast_call(
                sections, experts, half, images.reshape(tokens, width), norm_gain, slot_map.T, logit_scale,
                up_weight.reshape(hidden_units, width), down_weight.reshape(hidden_units, width),
            )
            return result.reshape(1, tokens, width)
        x_parts = 4
        result = pl.pallas_call(
            functools.partial(general_kernel, sections, experts, chunk),
            out_shape=pltpu.VMEM((tokens, width), bf16),
            in_specs=[hbm, hbm, hbm, pl.BlockSpec(memory_space=pltpu.HBM), hbm, hbm],
            out_specs=vmem,
            scratch_shapes=[
                pltpu.VMEM((width,), bf16),
                pltpu.VMEM((slots, width), bf16),
                pltpu.SMEM((1,), jnp.float32),
                pltpu.VMEM((tokens, width), bf16),
                pltpu.VMEM((tokens, width), bf16),
                pltpu.VMEM((tokens, 128), jnp.float32),
                pltpu.VMEM((hidden_units, width), bf16),
                pltpu.VMEM((hidden_units, width), bf16),
                pltpu.VMEM((experts, 2, half), bf16),
                pltpu.VMEM((n, 2, half), bf16),
                pltpu.VMEM((n, 2, half), bf16),
                pltpu.VMEM((n, 2, half), bf16),
                pltpu.SemaphoreType.DMA((3,)),
                pltpu.SemaphoreType.DMA((x_parts,)),
                pltpu.SemaphoreType.DMA((chunks,)),
                pltpu.SemaphoreType.DMA((chunks,)),
                pltpu.SemaphoreType.DMA((2,)),
                pltpu.SemaphoreType.DMA((2,)),
                pltpu.SemaphoreType.DMA((2,)),
            ],
            compiler_params=pltpu.CompilerParams(
                collective_id=0, has_side_effects=True, vmem_limit_bytes=60 * 1024 * 1024
            ),
        )(
            images.reshape(tokens, width), norm_gain, slot_map.T, logit_scale,
            up_weight.reshape(hidden_units, width), down_weight.reshape(hidden_units, width),
        )
        return result.reshape(1, tokens, width)

    return jax.shard_map(
        local,
        mesh=mesh,
        in_specs=(
            P(("section", "expert"), None, None),
            P(),
            P(),
            P(),
            P("expert", "section", None),
            P("expert", "section", None),
        ),
        out_specs=P(("section", "expert"), None, None),
        check_vma=False,
    )
```

```python
import functools

import jax
import jax.numpy as jnp
from jax import lax
from jax.experimental import pallas as pl
from jax.experimental.pallas import tpu as pltpu
from jax.sharding import PartitionSpec as P

epsilon = 1e-06
MESH = pl.DeviceIdType.MESH
NT = (((1,), (1,)), ((), ()))
TN = (((0,), (0,)), ((), ()))
U = 256
STRIP = 16


def split_of(total, most, unit):
    best = unit
    for size in range(unit, most + 1, unit):
        if total % size == 0:
            best = size
    return best


def far_first(sections, experts):
    def distance(k):
        mask = k % experts
        return -(k // experts + mask // 4 + mask // 2 % 2)

    return sorted(range(1, sections * experts), key=distance)


def swap_pairs(v, even):
    return jnp.where(even, pltpu.roll(v, v.shape[0] - 1, 0), pltpu.roll(v, 1, 0))

def gelu(x):
    k = 0.7978845608028654
    return (0.5 * x) * (1.0 + jnp.tanh(x * (k + (k * 0.044715) * (x * x))))

def stage_first(upt_v, half):
    hidden = upt_v.shape[1]
    for t in range(2):
        for q in range(2):
            pltpu.matmul_push_rhs(upt_v[pl.ds(t * U, U), pl.ds(q * hidden // 2, U)], t, q)


def expert_mlp(rows_ref, upt_v, down_v, act_v, out_ref, ups, downs, halves, half, width, lag=2):
    M = rows_ref.shape[0]
    hidden = upt_v.shape[1]
    bf16 = jnp.bfloat16
    right = width - half
    blocks = hidden // U // 2
    rem = right % U
    tiles = [(0, j * U) for j in range(half // U)] + [(1, j * U) for j in range(right // U)]
    tail = right // U * U
    strips = M // STRIP
    even = lax.broadcasted_iota(jnp.int32, (M, U), 0) % 2 == 0
    even_strip = lax.broadcasted_iota(jnp.int32, (STRIP, U), 0) % 2 == 0
    zero = jnp.zeros((M, U), bf16)
    slot = [0, 0]
    staged = [2, 2]

    def piece(s):
        return slice(s * STRIP, (s + 1) * STRIP)

    def feed(q, tile, accs, operands):
        r = slot[q]
        slot[q] = 1 - r
        if staged[q]:
            staged[q] -= 1
        else:
            pltpu.matmul_push_rhs(tile, r, q)
        first = True
        for acc, operand in zip(accs, operands):
            for s in range(strips):
                pltpu.matmul_acc_lhs(acc[s], operand[piece(s)], load_staged_rhs=r if first else None)
                first = False

    def at_block(q, b):
        return pl.ds((q * blocks + b) * U, U)

    lhs = []
    for side, at in tiles:
        v = rows_ref[:, at:at + U]
        lhs.append(jnp.where(even, v, zero) if side == 0 else jnp.where(even, zero, v))
    if rem:
        v = rows_ref[:, tail:tail + rem]
        v = jnp.where(even[:, :rem], zero[:, :rem], v)
        lhs_tail = [jnp.concatenate([v, zero[:, :rem]], axis=1), jnp.concatenate([zero[:, :rem], v], axis=1)]

    def finish(q, b, s):
        pre = pltpu.matmul_pop(ups[q][b][s])
        pre = pre + swap_pairs(pre, even_strip)
        act_v[piece(s), at_block(q, b)] = gelu(pre).astype(bf16)

    pending = []

    def drain(count):
        for _ in range(min(count, len(pending))):
            pending.pop(0)()

    def up_block(b, rate):
        for side_at, operand in zip(tiles, lhs):
            side, at = side_at
            for q in range(2):
                feed(q, upt_v[pl.ds(side * half + at, U), at_block(q, b)], [ups[q][b]], [operand])
            drain(rate)
        done = []
        if rem:
            k = pl.ds(half + tail, rem)
            if b % 2 == 1:
                for q in range(2):
                    pair = jnp.concatenate([upt_v[k, at_block(q, b - 1)], upt_v[k, at_block(q, b)]], axis=0)
                    feed(q, pair, [ups[q][b - 1], ups[q][b]], lhs_tail)
                done = [b - 1, b]
            elif b == blocks - 1:
                for q in range(2):
                    one = upt_v[k, at_block(q, b)]
                    feed(q, jnp.concatenate([one, one], axis=0), [ups[q][b]], lhs_tail[:1])
                done = [b]
        else:
            done = [b]
        for d in done:
            for s in range(strips):
                for q in range(2):
                    pending.append(lambda q=q, d=d, s=s: finish(q, d, s))

    for b in range(blocks):
        up_block(b, lag)

    def act(q, b):
        return act_v[:, at_block(q, b)]

    def down_step(j, b):
        side, at = tiles[j]
        for q in range(2):
            feed(q, down_v[at_block(q, b), pl.ds(side * half + at, U)], [downs[q][j]], [act(q, b)])

    def down_tail(pair):
        cols = pl.ds(half + tail, rem)
        for q in range(2):
            v = [down_v[at_block(q, b), cols] for b in pair]
            if len(v) == 1:
                v = v * 2
            feed(q, jnp.concatenate(v, axis=1), [halves[q][i] for i in range(len(pair))], [act(q, b) for b in pair])

    nl, nr = half // U, right // U
    pairs = [list(range(b, min(b + 2, blocks))) for b in range(0, blocks, 2)]

    def total(group, s):
        return pltpu.matmul_pop(group[0][s]) + pltpu.matmul_pop(group[1][s])

    def emit(j, s):
        l = total([downs[0][j], downs[1][j]], s)
        rows = piece(s)
        if j < nr:
            r = total([downs[0][nl + j], downs[1][nl + j]], s)
            out_ref[rows, j * U:(j + 1) * U] = jnp.where(even_strip, l, r).astype(bf16)
        elif rem:
            r = total([halves[0][0], halves[1][0]], s)[:, :rem] + total([halves[0][1], halves[1][1]], s)[:, rem:]
            both = jnp.where(even_strip[:, :rem], l[:, :rem], r)
            out_ref[rows, j * U:(j + 1) * U] = jnp.concatenate([both, l[:, rem:]], axis=1).astype(bf16)
        else:
            out_ref[rows, j * U:(j + 1) * U] = l.astype(bf16)

    ready = blocks - 1 if blocks % 2 else blocks - 2
    groups = []
    for j in reversed(range(nl)):
        groups.append((j, [j] + ([nl + j] if j < nr else [])))
    first = True
    for j, columns in groups:
        tails = rem and j >= nr
        for b in range(blocks):
            if first and b == ready:
                drain(len(pending))
            for c in columns:
                down_step(c, b)
                drain(lag)
            if tails and (b % 2 == 1 or b == blocks - 1):
                down_tail(pairs[b // 2])
                drain(lag)
        drain(len(pending))
        first = False
        for s in range(strips):
            pending.append(lambda j=j, s=s: emit(j, s))
    drain(len(pending))

def routing_kernel(
    sections, experts, half,
    x_hbm, gain_hbm, slot_hbm, scale_ref, up_hbm, down_hbm,
    xs, back, mix_left, mix_right,
    gain_ref, slot_ref, normed, stat, up_v, upt_v, down_v, act_v, send1, recv1, send2, recv2, sized,
    small_sem, x_sem, up_sem, down_sem, local_sem, send_sem, recv_sem,
):
    tokens, width = xs.shape
    slots = slot_ref.shape[0]
    padded = normed.shape[1]
    columns = padded // U
    images = sections * experts

    def spec(rows):
        return lambda q: [pltpu.ACC(q)((STRIP, U), jnp.float32) for _ in range(rows // STRIP)]

    def per_unit(count, rows):
        make = spec(rows)
        return [[make(q) for _ in range(count)] for q in range(2)]

    hidden = up_v.shape[0]
    wide = half // U + (width - half) // U

    def run(raws, ins, ups, downs, halves):
        routing_body(
            sections, experts, half,
            x_hbm, gain_hbm, slot_hbm, scale_ref, up_hbm, down_hbm,
            xs, back, mix_left, mix_right,
            gain_ref, slot_ref, normed, stat, up_v, upt_v, down_v, act_v, send1, recv1, send2, recv2, sized,
            small_sem, x_sem, up_sem, down_sem, local_sem, send_sem, recv_sem,
            raws, ins, ups, downs, halves,
        )

    pl.run_scoped(
        run,
        [pltpu.ACC(q)((slots, U), jnp.float32) for q in range(2)],
        [pltpu.ACC(t % 2)((2 * slots, U), jnp.float32) for t in range(columns)],
        per_unit(hidden // U // 2, 2 * images),
        per_unit(wide, 2 * images),
        per_unit(2, 2 * images),
    )


def routing_body(
    sections, experts, half,
    x_hbm, gain_hbm, slot_hbm, scale_ref, up_hbm, down_hbm,
    xs, back, mix_left, mix_right,
    gain_ref, slot_ref, normed, stat, up_v, upt_v, down_v, act_v, send1, recv1, send2, recv2, sized,
    small_sem, x_sem, up_sem, down_sem, local_sem, send_sem, recv_sem,
    raws, ins, ups, downs, halves,
):
    n = sections * experts
    tokens, width = xs.shape
    slots = slot_ref.shape[0]
    padded = normed.shape[1]
    hidden = up_v.shape[0]
    bf16 = jnp.bfloat16
    section = lax.axis_index("section")
    expert = lax.axis_index("expert")
    me = section * experts + expert

    x_parts = x_sem.shape[0]
    x_rows = tokens // x_parts
    x_copies = [
        pltpu.make_async_copy(
            x_hbm.at[pl.ds(i * x_rows, x_rows)], xs.at[pl.ds(i * x_rows, x_rows)], x_sem.at[i]
        )
        for i in range(x_parts)
    ]
    small_copies = [
        pltpu.make_async_copy(gain_hbm, gain_ref, small_sem.at[0]),
        pltpu.make_async_copy(slot_hbm, slot_ref, small_sem.at[1]),
    ]

    barrier = pltpu.get_barrier_semaphore()

    def for_others(visit, between=None):
        for at, k in enumerate(far_first(sections, experts)):
            if at == 8 and between is not None:
                between()
            s = lax.rem(section + k // experts, sections)
            e = jnp.bitwise_xor(expert, k % experts)
            visit(s * experts + e, e, {"section": s, "expert": e})

    def greet(target, e, device):
        pl.semaphore_signal(barrier, inc=1, device_id=device, device_id_type=MESH)

    def start_inputs():
        for copy in x_copies + small_copies:
            copy.start()

    for_others(greet, start_inputs)

    up_parts, down_parts = up_sem.shape[0], down_sem.shape[0]
    up_rows, down_rows = hidden // up_parts, hidden // down_parts

    def up_copy(c):
        rows = pl.ds(pl.multiple_of(c * up_rows, up_rows), up_rows)
        return pltpu.make_async_copy(up_hbm.at[rows], up_v.at[rows], up_sem.at[c])

    def down_copy(c):
        rows = pl.ds(c * down_rows, down_rows)
        return pltpu.make_async_copy(down_hbm.at[rows], down_v.at[rows], down_sem.at[c])

    for c in range(up_parts):
        up_copy(c).start()
    for c in range(down_parts):
        down_copy(c).start()

    for copy in small_copies:
        copy.wait()
    slot_rows = slot_ref[...]
    slot_wide = slot_rows.astype(jnp.float32)
    column_norm = jnp.sqrt(jnp.sum(slot_wide * slot_wide, axis=-1, keepdims=True) + epsilon)
    gain = gain_ref[...].astype(jnp.float32).reshape(1, width)
    if padded > width:
        normed[:, width:] = jnp.zeros((tokens, padded - width), bf16)
        slot_rows = jnp.concatenate([slot_rows, jnp.zeros((slots, padded - width), bf16)], axis=1)

    step_rows = 16

    def norm_step(i, carry):
        rows = pl.ds(pl.multiple_of(i * step_rows, step_rows), step_rows)
        values = xs[rows, :].astype(jnp.float32)
        spread = jnp.sum(values * values, axis=-1, keepdims=True) * (1.0 / width)
        result = (values * lax.rsqrt(spread + epsilon) * gain).astype(bf16)
        normed[rows, :width] = result
        wide = result.astype(jnp.float32)
        square = jnp.sum(wide * wide, axis=-1, keepdims=True)
        stat[rows, :] = jnp.broadcast_to(square, (step_rows, stat.shape[1]))
        return carry

    per = x_rows // step_rows
    for i, copy in enumerate(x_copies):
        copy.wait()
        lax.fori_loop(i * per, (i + 1) * per, norm_step, 0, unroll=True)

    tiles = padded // U
    for t in range(tiles):
        q, r = t % 2, t // 2 % 2
        pltpu.matmul_push_rhs(normed[:, t * U:(t + 1) * U], r, q, transpose=True)
        pltpu.matmul_acc_lhs(raws[q], slot_rows[:, t * U:(t + 1) * U], load_staged_rhs=r)
    raw = pltpu.matmul_pop(raws[0]) + pltpu.matmul_pop(raws[1])
    token_norm = jnp.sqrt(jnp.transpose(stat[...])[0:1, :] + epsilon)
    logits = scale_ref[0] * raw / (token_norm * column_norm)
    scores = jnp.exp(logits)
    dispatch = scores / jnp.sum(scores, axis=1, keepdims=True)
    combine = scores / jnp.sum(scores, axis=0, keepdims=True)
    dispatch = jnp.repeat(dispatch, 2, axis=0).astype(bf16)
    even = lax.broadcasted_iota(jnp.int32, (2 * slots, U), 0) % 2 == 0
    shift = tiles // 2
    for j in range(shift):
        for t in (j, j + shift):
            q, r = t % 2, t // 2 % 2
            pltpu.matmul_push_rhs(normed[:, t * U:(t + 1) * U], r, q)
            pltpu.matmul_acc_lhs(ins[t], dispatch, load_staged_rhs=r)
    for j in range(shift):
        left, right = pltpu.matmul_pop(ins[j]), pltpu.matmul_pop(ins[j + shift])
        send1[:, j * U:(j + 1) * U] = jnp.where(even, left, right).astype(bf16)

    pl.semaphore_wait(barrier, n - 1)

    def pair(index):
        return pl.ds(pl.multiple_of(2 * index, 2), 2)

    def send_rows(source, target, i, by_expert):
        def visit(index, e, device):
            pltpu.make_async_remote_copy(
                src_ref=source.at[pair(e if by_expert else index)], dst_ref=target.at[pair(me)],
                send_sem=send_sem.at[i], recv_sem=recv_sem.at[i],
                device_id=device, device_id_type=MESH,
            ).start()

        for_others(visit)

    def wait_all(sem):
        pltpu.make_async_copy(sized, sized, sem).wait()

    send_rows(send1, recv1, 0, True)
    own1 = pltpu.make_async_copy(send1.at[pair(expert)], recv1.at[pair(me)], local_sem.at[0])
    own1.start()

    stacked = jnp.concatenate([jnp.repeat(combine, 2, axis=0)] * sections, axis=0)
    by_token = jnp.transpose(stacked)
    lane_even = lax.broadcasted_iota(jnp.int32, by_token.shape, 1) % 2 == 0
    mix_left[...] = jnp.where(lane_even, by_token, 0.0).astype(bf16)
    mix_right[...] = jnp.where(lane_even, 0.0, by_token).astype(bf16)

    def turn(c, carry):
        up_copy(c).wait()
        at = pl.multiple_of(c * up_rows, up_rows)
        for k in range(0, width, 128):
            upt_v[k:k + 128, pl.ds(at, up_rows)] = up_v[pl.ds(at, up_rows), k:k + 128].T
        return carry

    lax.fori_loop(0, up_parts, turn, 0)
    for c in range(down_parts):
        down_copy(c).wait()

    stage_first(upt_v, half)
    own1.wait()
    wait_all(recv_sem.at[0])
    expert_mlp(recv1, upt_v, down_v, act_v, send2, ups, downs, halves, half, width)

    send_rows(send2, recv2, 1, False)
    own2 = pltpu.make_async_copy(send2.at[pair(me)], recv2.at[pair(me)], local_sem.at[1])
    own2.start()
    wait_all(send_sem.at[0])
    own2.wait()
    wait_all(recv_sem.at[1])
    back[...] = recv2[...]
    wait_all(send_sem.at[1])


def mixing_kernel(half, xs, back, mix_left, mix_right, out_hbm, out_v, sem):
    tokens, width = xs.shape
    parts = sem.shape[0]
    rows_each = tokens // parts
    copies = []
    for i in range(parts):
        rows = pl.ds(i * rows_each, rows_each)
        left = jnp.dot(mix_left[rows, :], back[...], preferred_element_type=jnp.float32)
        right = jnp.dot(mix_right[rows, :], back[:, :width - half], preferred_element_type=jnp.float32)
        out_v[rows, :half] = (xs[rows, :half].astype(jnp.float32) + left).astype(jnp.bfloat16)
        out_v[rows, half:] = (xs[rows, half:].astype(jnp.float32) + right).astype(jnp.bfloat16)
        copy = pltpu.make_async_copy(out_v.at[rows], out_hbm.at[rows], sem.at[i])
        copy.start()
        copies.append(copy)
    for copy in copies:
        copy.wait()


def fast_call(sections, experts, half, images, norm_gain, slot_map, logit_scale, up_weight, down_weight):
    tokens, width = images.shape
    hidden = up_weight.shape[0]
    slots = slot_map.shape[0]
    n = sections * experts
    padded = -(-width // (2 * U)) * 2 * U
    bf16 = jnp.bfloat16
    hbm = pl.BlockSpec(memory_space=pl.ANY)
    vmem = pl.BlockSpec(memory_space=pltpu.VMEM)
    x_parts, up_parts, down_parts, out_parts = 4, hidden // U, 2, 4
    xs, back, mix_left, mix_right = pl.pallas_call(
        functools.partial(routing_kernel, sections, experts, half),
        out_shape=[
            pltpu.VMEM((tokens, width), bf16),
            pltpu.VMEM((2 * n, half), bf16),
            pltpu.VMEM((tokens, 2 * n), bf16),
            pltpu.VMEM((tokens, 2 * n), bf16),
        ],
        in_specs=[hbm, hbm, hbm, pl.BlockSpec(memory_space=pltpu.SMEM), hbm, hbm],
        out_specs=[vmem] * 4,
        scratch_shapes=[
            pltpu.VMEM((width,), bf16),
            pltpu.VMEM((slots, width), bf16),
            pltpu.VMEM((tokens, padded), bf16),
            pltpu.VMEM((tokens, 128), jnp.float32),
            pltpu.VMEM((hidden, width), bf16),
            pltpu.VMEM((width, hidden), bf16),
            pltpu.VMEM((hidden, width), bf16),
            pltpu.VMEM((2 * n, hidden), bf16),
            pltpu.VMEM((2 * slots, half), bf16),
            pltpu.VMEM((2 * n, half), bf16),
            pltpu.VMEM((2 * n, half), bf16),
            pltpu.VMEM((2 * n, half), bf16),
            pltpu.VMEM((n - 1, 2, half), bf16),
            pltpu.SemaphoreType.DMA((2,)),
            pltpu.SemaphoreType.DMA((x_parts,)),
            pltpu.SemaphoreType.DMA((up_parts,)),
            pltpu.SemaphoreType.DMA((down_parts,)),
            pltpu.SemaphoreType.DMA((2,)),
            pltpu.SemaphoreType.DMA((2,)),
            pltpu.SemaphoreType.DMA((2,)),
        ],
        compiler_params=pltpu.CompilerParams(
            collective_id=0, has_side_effects=True, vmem_limit_bytes=60 * 1024 * 1024
        ),
    )(images, norm_gain, slot_map, logit_scale, up_weight, down_weight)
    return pl.pallas_call(
        functools.partial(mixing_kernel, half),
        out_shape=jax.ShapeDtypeStruct((tokens, width), bf16),
        in_specs=[vmem] * 4,
        out_specs=hbm,
        scratch_shapes=[pltpu.VMEM((tokens, width), bf16), pltpu.SemaphoreType.DMA((out_parts,))],
    )(*(pltpu.with_memory_space_constraint(v, pltpu.VMEM) for v in (xs, back, mix_left, mix_right)))


def general_kernel(
    sections, experts, chunk,
    x_hbm, gain_hbm, slot_hbm, scale_hbm, up_hbm, down_hbm,
    out_v,
    gain_ref, slot_ref, scale_ref, xs, normed, stat, up_v, down_v, send1, recv1, send2, recv2,
    small_sem, x_sem, up_sem, down_sem, local_sem, send_sem, recv_sem,
):
    n = sections * experts
    tokens, width = xs.shape
    half = send1.shape[2]
    rest = width - half
    hidden_units = up_v.shape[0]
    chunks = hidden_units // chunk
    section = lax.axis_index("section")
    expert = lax.axis_index("expert")
    me = section * experts + expert

    x_parts = x_sem.shape[0]
    x_rows = tokens // x_parts
    x_copies = [
        pltpu.make_async_copy(
            x_hbm.at[pl.ds(i * x_rows, x_rows)], xs.at[pl.ds(i * x_rows, x_rows)], x_sem.at[i]
        )
        for i in range(x_parts)
    ]
    small_copies = [
        pltpu.make_async_copy(source, target, small_sem.at[i])
        for i, (source, target) in enumerate(
            [(gain_hbm, gain_ref), (slot_hbm, slot_ref), (scale_hbm, scale_ref)]
        )
    ]

    barrier = pltpu.get_barrier_semaphore()

    def wrapped(value, bound):
        return jnp.where(value >= bound, value - bound, value)

    def visit_at(k, visit):
        s = wrapped(section + k // experts, sections)
        mask = k % experts
        e = jnp.bitwise_xor(expert, mask) if paired else wrapped(expert + mask, experts)
        visit(s * experts + e, e, {"section": s, "expert": e})

    paired = experts & (experts - 1) == 0
    order = far_first(sections, experts)

    def for_others(visit, between=None):
        if n <= 64:
            for at, k in enumerate(order):
                if at == 8 and between is not None:
                    between()
                visit_at(k, visit)
        else:
            if between is not None:
                between()

            def step(k, carry):
                visit_at(k, visit)
                return carry

            lax.fori_loop(1, n, step, 0)

    def greet(target, e, device):
        pl.semaphore_signal(barrier, inc=1, device_id=device, device_id_type=MESH)

    def start_inputs():
        for copy in x_copies + small_copies:
            copy.start()

    for_others(greet, start_inputs)

    up_copies = []
    down_copies = []
    for c in range(chunks):
        rows = pl.ds(c * chunk, chunk)
        up_copies.append(pltpu.make_async_copy(up_hbm.at[rows], up_v.at[rows], up_sem.at[c]))
        down_copies.append(pltpu.make_async_copy(down_hbm.at[rows], down_v.at[rows], down_sem.at[c]))
    for copy in up_copies + down_copies:
        copy.start()

    for copy in small_copies:
        copy.wait()
    columns = slot_ref[...].astype(jnp.float32)
    column_norm = jnp.sqrt(jnp.sum(columns * columns, axis=-1, keepdims=True) + epsilon)
    gain = gain_ref[...].astype(jnp.float32).reshape(1, width)

    step_rows = 16

    def norm_step(i, carry):
        rows = pl.ds(pl.multiple_of(i * step_rows, step_rows), step_rows)
        values = xs[rows, :].astype(jnp.float32)
        spread = jnp.sum(values * values, axis=-1, keepdims=True) * (1.0 / width)
        result = (values * lax.rsqrt(spread + epsilon) * gain).astype(jnp.bfloat16)
        normed[rows, :] = result
        wide = result.astype(jnp.float32)
        square = jnp.sum(wide * wide, axis=-1, keepdims=True)
        stat[rows, :] = jnp.broadcast_to(square, (step_rows, stat.shape[1]))
        return carry

    per = x_rows // step_rows
    for i, copy in enumerate(x_copies):
        copy.wait()
        lax.fori_loop(i * per, (i + 1) * per, norm_step, 0, unroll=True)

    raw = lax.dot_general(slot_ref[...], normed[...], NT, preferred_element_type=jnp.float32)
    token_norm = jnp.sqrt(jnp.transpose(stat[...])[0:1, :] + epsilon)
    logits = scale_ref[0] * raw / (token_norm * column_norm)
    scores = jnp.exp(logits)
    dispatch = (scores / jnp.sum(scores, axis=1, keepdims=True)).astype(jnp.bfloat16)
    combine = (scores / jnp.sum(scores, axis=0, keepdims=True)).astype(jnp.bfloat16)
    slot_in = jnp.dot(dispatch, normed[...], preferred_element_type=jnp.float32).astype(jnp.bfloat16)
    send1[:, 0, :] = slot_in[:, :half]
    send1[:, 1, :rest] = slot_in[:, half:]

    pl.semaphore_wait(barrier, n - 1)

    own1 = pltpu.make_async_copy(send1.at[expert], recv1.at[me], local_sem.at[0])
    own1.start()

    def dispatch_row(target, e, device):
        pltpu.make_async_remote_copy(
            src_ref=send1.at[e], dst_ref=recv1.at[me], send_sem=send_sem.at[0], recv_sem=recv_sem.at[0],
            device_id=device, device_id_type=MESH,
        ).start()

    for_others(dispatch_row)

    def wait_all(buffer, sem):
        part = buffer.at[pl.ds(0, n - 1)]
        pltpu.make_async_copy(part, part, sem).wait()

    own1.wait()
    wait_all(recv1, recv_sem.at[0])
    left = recv1[:, 0, :]
    right = recv1[:, 1, :rest]
    rows_in = jnp.concatenate([left, right], axis=1)
    total = None
    for c in range(chunks):
        rows = pl.ds(c * chunk, chunk)
        up_copies[c].wait()
        pre = lax.dot_general(rows_in, up_v[rows, :], NT, preferred_element_type=jnp.float32)
        act = jax.nn.gelu(pre).astype(jnp.bfloat16)
        down_copies[c].wait()
        term = jnp.dot(act, down_v[rows, :], preferred_element_type=jnp.float32)
        total = term if total is None else total + term
    partial = total.astype(jnp.bfloat16)
    send2[:, 0, :] = partial[:, :half]
    send2[:, 1, :rest] = partial[:, half:]

    own2 = pltpu.make_async_copy(send2.at[me], recv2.at[me], local_sem.at[1])
    own2.start()

    def return_row(target, e, device):
        pltpu.make_async_remote_copy(
            src_ref=send2.at[target], dst_ref=recv2.at[me], send_sem=send_sem.at[1], recv_sem=recv_sem.at[1],
            device_id=device, device_id_type=MESH,
        ).start()

    for_others(return_row)

    own2.wait()
    wait_all(recv2, recv_sem.at[1])
    summed = recv2[pl.ds(0, experts)].astype(jnp.float32)
    for s in range(1, sections):
        summed = summed + recv2[pl.ds(s * experts, experts)].astype(jnp.float32)
    slot_out = summed.astype(jnp.bfloat16)
    slot_out = jnp.concatenate([slot_out[:, 0, :], slot_out[:, 1, :rest]], axis=1)

    o_parts = 4
    o_rows = tokens // o_parts
    for i in range(o_parts):
        rows = pl.ds(i * o_rows, o_rows)
        mixed = lax.dot_general(
            combine[:, i * o_rows:(i + 1) * o_rows], slot_out, TN, preferred_element_type=jnp.float32
        )
        out_v[rows, :] = (xs[rows, :].astype(jnp.float32) + mixed).astype(jnp.bfloat16)
    wait_all(recv1, send_sem.at[0])
    wait_all(recv2, send_sem.at[1])


def solution(mesh):
    sections, experts = mesh.shape["section"], mesh.shape["expert"]
    n = sections * experts

    def local(images, norm_gain, slot_map, logit_scale, up_weight, down_weight):
        count, tokens, width = images.shape
        held, hidden_units, _ = up_weight.shape
        slots = slot_map.shape[1]
        assert count == 1 and held == 1 and slots == experts
        half = -(-width // 256) * 128
        chunk = split_of(hidden_units, 1280, 128)
        chunks = hidden_units // chunk
        bf16 = jnp.bfloat16
        hbm = pl.BlockSpec(memory_space=pl.ANY)
        vmem = pl.BlockSpec(memory_space=pltpu.VMEM)
        fits = (
            tokens == U and slots % STRIP == 0 and experts & (experts - 1) == 0 and 2 * n <= 64
            and half % U == 0 and half >= 2 * U and 2 * half - width < U and hidden_units % (2 * U) == 0
        )
        if fits:
            result = fast_call(
                sections, experts, half, images.reshape(tokens, width), norm_gain, slot_map.T, logit_scale,
                up_weight.reshape(hidden_units, width), down_weight.reshape(hidden_units, width),
            )
            return result.reshape(1, tokens, width)
        x_parts = 4
        result = pl.pallas_call(
            functools.partial(general_kernel, sections, experts, chunk),
            out_shape=pltpu.VMEM((tokens, width), bf16),
            in_specs=[hbm, hbm, hbm, pl.BlockSpec(memory_space=pltpu.HBM), hbm, hbm],
            out_specs=vmem,
            scratch_shapes=[
                pltpu.VMEM((width,), bf16),
                pltpu.VMEM((slots, width), bf16),
                pltpu.SMEM((1,), jnp.float32),
                pltpu.VMEM((tokens, width), bf16),
                pltpu.VMEM((tokens, width), bf16),
                pltpu.VMEM((tokens, 128), jnp.float32),
                pltpu.VMEM((hidden_units, width), bf16),
                pltpu.VMEM((hidden_units, width), bf16),
                pltpu.VMEM((experts, 2, half), bf16),
                pltpu.VMEM((n, 2, half), bf16),
                pltpu.VMEM((n, 2, half), bf16),
                pltpu.VMEM((n, 2, half), bf16),
                pltpu.SemaphoreType.DMA((3,)),
                pltpu.SemaphoreType.DMA((x_parts,)),
                pltpu.SemaphoreType.DMA((chunks,)),
                pltpu.SemaphoreType.DMA((chunks,)),
                pltpu.SemaphoreType.DMA((2,)),
                pltpu.SemaphoreType.DMA((2,)),
                pltpu.SemaphoreType.DMA((2,)),
            ],
            compiler_params=pltpu.CompilerParams(
                collective_id=0, has_side_effects=True, vmem_limit_bytes=60 * 1024 * 1024
            ),
        )(
            images.reshape(tokens, width), norm_gain, slot_map.T, logit_scale,
            up_weight.reshape(hidden_units, width), down_weight.reshape(hidden_units, width),
        )
        return result.reshape(1, tokens, width)

    return jax.shard_map(
        local,
        mesh=mesh,
        in_specs=(
            P(("section", "expert"), None, None),
            P(),
            P(),
            P(),
            P("expert", "section", None),
            P("expert", "section", None),
        ),
        out_specs=P(("section", "expert"), None, None),
        check_vma=False,
    )
```
